32 devices in a mesh: dp: 8 (over z, y), tensor: 4 (over x, core).
Axes of the slice: x: 2, y: 2, z: 4, core: 2. Of those that a mesh axis runs over, the one named last changes fastest.
Arguments:
- logits: bfloat16 [32, 64, 152064], P('dp', None, 'tensor'), may hold values from -3 to 3
- tokens: int32 [32, 64], P('dp'), may hold values from 0 to 152063
- lengths: int32 [32], P('dp'), may hold values from 1 to 64, 1024 in all
- group_ids: int32 [32], P('dp'), may hold values from 0 to 1, as said below
- rewards: float32 [32], P('dp'), may hold values from -4 to 4
- old_logp: float32 [32, 64], P('dp'), may hold values from -12.6 to -11.5
- ref_logp: float32 [32, 64], P('dp'), may hold values from -12.6 to -11.5
Outputs:
- token_logp: float32 [32, 64], P('dp')
- advantages: float32 [32], P('dp')
- seq_loss: float32 [32], P('dp')
- total_loss: float32 [], replicated
The draws below stay inside these ranges and needn't reach their ends.
Inputs may be any that keep to these rules, and one draw needn't show every extreme that they name: `group_ids`: each number 0 to 1 names exactly 16 responses, placed at random over the batch. `lengths`: each response has 1 to 64 tokens, the longest exactly 64.
All inputs are finite; a program needn't handle non-finite values.
Results may differ from the reference program's by a relative error of at most 0.0003.
Values sent between devices are 32-bit elements.
A program may use at most 128 MiB of HBM per device.

```python
import math
import jax
import jax.numpy as jnp
import numpy as np
from jax import lax

VOCAB = 152064
SEQ = 64
GROUP = 16
RESPONSES = 32
GROUPS = 2


def draw_group_ids(key, part):
    order = jax.random.permutation(key, RESPONSES)
    return (order // GROUP).astype(jnp.int32)


def touch_ends(array, rng, smallest, largest):
    longest = array.shape.index(max(array.shape))
    spots = []
    for shift in (0, 1):
        where = [jax.random.randint(jax.random.fold_in(rng, axis), (), 0, length) for axis, length in enumerate(array.shape)]
        where[longest] = (where[longest] + shift) % array.shape[longest]
        spots.append(tuple(where))
    return array.at[spots[0]].set(smallest).at[spots[1]].set(largest)


def block_levels(key, extent, cuts, low, largest):
    def one(position, parts):
        steps = jax.random.uniform(jax.random.fold_in(jax.random.fold_in(key, 6), position), (parts,), jnp.float32, low / len(cuts), largest / len(cuts))
        return jnp.repeat(jnp.exp(steps), extent[position] // parts).reshape((-1,) + (1,) * (len(extent) - position - 1))

    loudness = one(*cuts[0])
    for cut in cuts[1:]:
        loudness = loudness * one(*cut)
    return loudness


def skewed_wide(key, dims, number_of, lean):
    loads = [min(1 << octave, number_of + 1 - (1 << octave)) * (1 << 20) // math.isqrt((1 << octave) ** lean) + 1 for octave in range((number_of + 1).bit_length()) if 1 << octave <= number_of]
    scale = 1 + sum(loads) // (1 << 30)
    table = np.cumsum(np.array([max(1, weight // scale) for weight in loads]))
    pick = jax.random.randint(jax.random.fold_in(key, 1), dims, 0, int(table[len(loads) - 1]))
    start = jnp.left_shift(1, jnp.searchsorted(jnp.asarray(table, jnp.int32), pick, side="right").astype(jnp.int32))
    standing = start - 1 + jax.random.randint(jax.random.fold_in(key, 4), dims, 0, 1 << 30) % jnp.minimum(start, number_of + 1 - start)
    return jax.random.permutation(jax.random.fold_in(key, 2), number_of)[standing].astype(jnp.int32)


def profile(number_of, total, reach, lean):
    portions = [(1 << 20) // math.isqrt(grade ** lean) + 1 for grade in range(2, number_of + 1)]
    surplus, holding = total - reach - (number_of - 1), [1] * (number_of - 1)
    while surplus > 0:
        candidates = [i for i in range(number_of - 1) if holding[i] < reach]
        whole, budget = sum([portions[i] for i in candidates]), surplus
        for i in candidates:
            more = min(reach - holding[i], max(1, budget * portions[i] // whole), surplus)
            holding[i] = holding[i] + more
            surplus = surplus - more
    return np.array([reach] + holding)


def uneven_parts(own_key, count, total, limit, lean):
    if count == 2:
        one = jax.random.randint(own_key, (), max(1, total - limit), min(limit, total - 1) + 1)
        return jnp.stack([one, total - one])
    sizes = jnp.asarray(profile(count, total, limit, lean), jnp.int32)
    twos = (count - 1) // 2
    giver, sink = sizes[1:1 + 2 * twos:2], sizes[2:2 + 2 * twos:2]
    room = jnp.minimum(giver - 1, limit - sink)
    shifted = jax.random.randint(jax.random.fold_in(own_key, 1), (twos,), 0, 1 << 20) % (room + 1)
    sizes = sizes.at[1:1 + 2 * twos:2].set(giver - shifted).at[2:2 + 2 * twos:2].set(sink + shifted)
    return sizes[jax.random.permutation(jax.random.fold_in(own_key, 2), count)]


def normal_values(rng, extent, width, most, cuts=(), kind=jnp.bfloat16):
    values = width * jax.random.normal(rng, extent, jnp.float32)
    if cuts:
        values = values * block_levels(rng, extent, cuts, -0.22, 0.18)
    return jnp.clip(values, -most, most).astype(kind)


def setup_inputs(seed: int = 0) -> dict:
    key_list = jax.random.split(jax.random.key(seed), 8)
    logits = normal_values(key_list[0], (RESPONSES, SEQ, VOCAB), 0.5, 3.0, ((0, 8), (2, 4)))
    tokens = touch_ends(skewed_wide(key_list[1], (RESPONSES, SEQ), VOCAB, 2), jax.random.fold_in(key_list[1], 3), 0, VOCAB - 1).astype(jnp.int32)
    lengths = uneven_parts(key_list[2], RESPONSES, RESPONSES * SEQ // 2, SEQ, 2).astype(jnp.int32)
    group_ids = draw_group_ids(jax.random.fold_in(key_list[7], 71), 0)
    rewards = normal_values(key_list[4], (RESPONSES,), 1.0, 4.0, ((0, 8),), jnp.float32)
    old_logp = jnp.clip(-12.6 + 1.1000004 * jax.random.uniform(key_list[5], (RESPONSES, SEQ), jnp.float32) ** block_levels(key_list[5], (RESPONSES, SEQ), ((0, 8),), -0.2, 0.2), -12.6, -11.5)
    ref_logp = jnp.clip(-12.6 + 1.1000004 * jax.random.uniform(key_list[6], (RESPONSES, SEQ), jnp.float32) ** block_levels(key_list[6], (RESPONSES, SEQ), ((0, 8),), -0.2, 0.2), -12.6, -11.5)
    return dict(logits=logits, tokens=tokens, lengths=lengths, group_ids=group_ids, rewards=rewards, old_logp=old_logp, ref_logp=ref_logp)


def row_logp(pair):
    rows, row_tokens = pair
    values = rows.astype(jnp.float32)
    row_peak = lax.optimization_barrier(jnp.max(values, axis=-1))
    row_total = lax.optimization_barrier(jnp.sum(jnp.exp(values - row_peak[:, None]), axis=-1))
    picked = jnp.take_along_axis(values, row_tokens[:, None].astype(jnp.int32), axis=-1)[:, 0]
    return picked - row_peak - jnp.log(row_total)

def reference(logits, tokens, lengths, group_ids, rewards, old_logp, ref_logp):
    raw_logp = lax.map(row_logp, (logits, tokens))
    positions = jnp.arange(SEQ, dtype=jnp.int32)[None, :]
    is_valid = positions < lengths[:, None]
    token_logp = jnp.where(is_valid, raw_logp, jnp.float32(0.0))
    group_sum = jax.ops.segment_sum(rewards, group_ids, num_segments=GROUPS)
    group_mean = group_sum / GROUP
    spread = rewards - group_mean[group_ids]
    squares = jax.ops.segment_sum(spread * spread, group_ids, num_segments=GROUPS)
    deviation = jnp.sqrt(squares / (GROUP - 1))
    advantages = spread / (deviation[group_ids] + 0.0001)
    prob_ratio = jnp.exp(token_logp - old_logp)
    clipped = jnp.clip(prob_ratio, 0.8, 1.28)
    token_gain = advantages[:, None]
    policy = -jnp.minimum(prob_ratio * token_gain, clipped * token_gain)
    ref_drift = ref_logp - token_logp
    penalty = jnp.exp(ref_drift) - ref_drift - 1.0
    token_terms = jnp.where(is_valid, policy + 0.04 * penalty, jnp.float32(0.0))
    seq_loss = lax.optimization_barrier(jnp.sum(token_terms, axis=1)) / lengths.astype(jnp.float32)
    total_loss = jnp.sum(seq_loss) / RESPONSES
    return (token_logp, advantages, seq_loss, total_loss)
```

```python
import functools
import math

import jax
import jax.numpy as jnp
from jax import lax
from jax.experimental import pallas as pl
from jax.experimental.pallas import tpu as pltpu
from jax.sharding import PartitionSpec as P

GROUP = 16
CLIP_LOW = 0.2
CLIP_HIGH = 0.28
KL_WEIGHT = 0.04
STD_EPS = 0.0001
LOG2E = math.log2(math.e)
STRIP = 16
LANES = 128
MESH = pl.DeviceIdType.MESH


def total_wait(ref, sem):
    pltpu.make_async_copy(ref, ref, sem).wait()


def strip_stats(block, width, offset):
    tiles = width // LANES
    step = max(u for u in range(1, 13) if tiles % u == 0)

    def body(k, state):
        total, picked = state
        first = k * (step * LANES)
        base = pl.multiple_of(first, LANES)
        parts = []
        for u in range(step):
            x = block[:, pl.ds(base + u * LANES, LANES)].astype(jnp.float32)
            picked = jnp.where(offset == first + u * LANES, x, picked)
            parts.append(jnp.exp2(x * LOG2E))
        while len(parts) > 1:
            parts = [sum(parts[i : i + 2][1:], parts[i]) for i in range(0, len(parts), 2)]
        return total + parts[0], picked

    zero = jnp.zeros((STRIP, LANES), jnp.float32)
    total, picked = lax.fori_loop(0, tiles // step, body, (zero, zero))
    tail = width - tiles * LANES
    if tail:
        x = block[:, tiles * LANES :].astype(jnp.float32)
        pad = jnp.zeros((STRIP, LANES - tail), jnp.float32)
        total = total + jnp.concatenate([jnp.exp2(x * LOG2E), pad], axis=1)
        x = jnp.concatenate([x, pad], axis=1)
        picked = jnp.where(offset == tiles * LANES, x, picked)
    return total, picked


def strip_offset(tokens, resp, first, start):
    rows = lax.broadcasted_iota(jnp.int32, (STRIP, LANES), 0)
    column = jnp.zeros((STRIP, LANES), jnp.int32)
    for r in range(STRIP):
        column = jnp.where(rows == r, tokens[resp, first + r] - start, column)
    return column - lax.broadcasted_iota(jnp.int32, (STRIP, LANES), 1)


def kernel(dims, *refs):
    dp, tp, resps, seq, width = dims
    count = dp * tp
    strips = seq // STRIP
    logits, tokens, lengths, group_ids, rewards, old, ref = refs[:7]
    out_logp, out_small = refs[7:9]
    refs = refs[9:]
    blocks = refs[: resps * strips]
    acc, early, head, last, joined, send_sem, recv_sem, load_sem = refs[resps * strips :]
    d, t = lax.axis_index("dp"), lax.axis_index("tensor")
    me = d * tp + t

    loads = []
    for i in range(resps):
        for s in range(strips):
            n = i * strips + s
            loads.append(
                pltpu.make_async_copy(logits.at[i, pl.ds(s * STRIP, STRIP), :], blocks[n], load_sem.at[n])
            )
            loads[-1].start()

    barrier = pltpu.get_barrier_semaphore()

    def peer(k):
        other = lax.rem(me + k, count)
        return (other // tp, lax.rem(other, tp))

    @pl.loop(1, count)
    def _(k):
        pl.semaphore_signal(barrier, inc=1, device_id=peer(k), device_id_type=MESH)

    lane_row = lax.broadcasted_iota(jnp.int32, (resps, LANES), 0)
    zero = jnp.zeros((resps, LANES), jnp.float32)
    spread_len, spread_rew, spread_gid = zero, zero, zero
    for i in range(resps):
        hit = lane_row == i
        spread_len = jnp.where(hit, lengths[i].astype(jnp.float32), spread_len)
        spread_rew = jnp.where(hit, rewards[i], spread_rew)
        spread_gid = jnp.where(hit, group_ids[i].astype(jnp.float32), spread_gid)
    early[d, 0] = spread_len
    early[d, 1] = spread_rew
    early[d, 2] = spread_gid
    early[d, 3] = jnp.concatenate([old[...], ref[...]], axis=1)

    start = t * width
    ones = jnp.ones((8, LANES), jnp.float32)

    def send_all(buf, which):
        @pl.loop(1, count)
        def _(k):
            pltpu.make_async_remote_copy(
                buf.at[me], buf.at[me], send_sem.at[which], recv_sem.at[which], device_id=peer(k), device_id_type=MESH
            ).start()

    for i in range(resps):
        for s in range(strips):
            n = i * strips + s
            loads[n].wait()
            total, picked = strip_stats(blocks[n], width, strip_offset(tokens, i, s * STRIP, start))
            acc[pl.ds(s * STRIP, STRIP)] = total
            acc[pl.ds(seq + s * STRIP, STRIP)] = picked
        line = lax.dot_general(
            ones, acc[...], (((1,), (1,)), ((), ())),
            precision=lax.Precision.HIGHEST, preferred_element_type=jnp.float32,
        )[:1]
        if i == 0:
            pl.semaphore_wait(barrier, count - 1)

            @pl.loop(1, dp)
            def _(k):
                pltpu.make_async_remote_copy(
                    early.at[d], early.at[d], send_sem.at[0], recv_sem.at[0],
                    device_id=(lax.rem(d + k, dp), t), device_id_type=MESH,
                ).start()

        if i < resps - 1:
            head[me, i] = line
            if i == resps - 2:
                send_all(head, 1)
        else:
            last[me] = line
            send_all(last, 2)

    total_wait(early.at[pl.ds(0, dp - 1)], recv_sem.at[0])
    length = early[:, 0]
    reward = early[:, 1]
    group = early[:, 2]
    old_all = early[:, 3]
    groups = resps * dp // GROUP
    mean_of = jnp.zeros_like(reward)
    for g in range(groups):
        hit = group == float(g)
        mean = jnp.sum(jnp.where(hit, reward, 0.0), axis=(0, 1), keepdims=True) / GROUP
        mean_of = jnp.where(hit, mean, mean_of)
    spread = reward - mean_of
    dev_of = jnp.zeros_like(reward)
    for g in range(groups):
        hit = group == float(g)
        squares = jnp.sum(jnp.where(hit, spread * spread, 0.0), axis=(0, 1), keepdims=True)
        dev_of = jnp.where(hit, jnp.sqrt(squares / (GROUP - 1)), dev_of)
    advantage = spread / (dev_of + STD_EPS)

    total_wait(head.at[pl.ds(0, count - 1)], recv_sem.at[1])
    total_wait(last.at[pl.ds(0, count - 1)], recv_sem.at[2])
    for a in range(dp):
        for i in range(resps):
            parts = [head[a * tp + b, i] if i < resps - 1 else last[a * tp + b] for b in range(tp)]
            joined[a, pl.ds(i, 1)] = functools.reduce(jnp.add, parts)
    joint = joined[...]
    position = lax.broadcasted_iota(jnp.int32, joint.shape, 2).astype(jnp.float32)
    valid = (position < length) & (position < seq)
    raw = pltpu.roll(joint, LANES - seq, 2) - jnp.log(joint)
    logp = jnp.where(valid, raw, 0.0)
    ratio = jnp.exp(logp - old_all)
    clipped = jnp.clip(ratio, 1.0 - CLIP_LOW, 1.0 + CLIP_HIGH)
    policy = -jnp.minimum(ratio * advantage, clipped * advantage)
    drift = pltpu.roll(old_all, LANES - seq, 2) - logp
    penalty = jnp.exp(drift) - drift - 1.0
    terms = jnp.where(valid, policy + KL_WEIGHT * penalty, 0.0)
    seq_loss = jnp.sum(terms, axis=2, keepdims=True) / length
    total = jnp.sum(seq_loss, axis=(0, 1), keepdims=True) / (resps * dp)
    joined[...] = logp
    out_logp[...] = joined[d][:, :seq]
    out_small[2] = jnp.broadcast_to(total[0], (resps, LANES))
    joined[...] = advantage
    out_small[0] = joined[d]
    joined[...] = seq_loss
    out_small[1] = joined[d]

    total_wait(early.at[pl.ds(0, dp - 1)], send_sem.at[0])
    total_wait(head.at[pl.ds(0, count - 1)], send_sem.at[1])
    total_wait(last.at[pl.ds(0, count - 1)], send_sem.at[2])


def solution(mesh):
    dp, tp = mesh.shape["dp"], mesh.shape["tensor"]

    def local(logits, tokens, lengths, group_ids, rewards, old_logp, ref_logp):
        resps, seq, width = logits.shape
        strips = seq // STRIP
        vmem = pl.BlockSpec(memory_space=pltpu.VMEM)
        smem = pl.BlockSpec(memory_space=pltpu.SMEM)
        logp, small = pl.pallas_call(
            functools.partial(kernel, (dp, tp, resps, seq, width)),
            out_shape=(
                jax.ShapeDtypeStruct((resps, seq), jnp.float32),
                jax.ShapeDtypeStruct((3, resps, LANES), jnp.float32),
            ),
            in_specs=[pl.BlockSpec(memory_space=pl.ANY), smem, smem, smem, smem, vmem, vmem],
            out_specs=(vmem, vmem),
            scratch_shapes=[pltpu.VMEM((STRIP, width), logits.dtype)] * (resps * strips)
            + [
                pltpu.VMEM((2 * seq, LANES), jnp.float32),
                pltpu.VMEM((dp, 4, resps, LANES), jnp.float32),
                pltpu.VMEM((dp * tp, resps - 1, 1, LANES), jnp.float32),
                pltpu.VMEM((dp * tp, 1, LANES), jnp.float32),
                pltpu.VMEM((dp, resps, LANES), jnp.float32),
                pltpu.SemaphoreType.DMA((3,)),
                pltpu.SemaphoreType.DMA((3,)),
                pltpu.SemaphoreType.DMA((resps * strips,)),
            ],
            compiler_params=pltpu.CompilerParams(
                collective_id=0, has_side_effects=True, vmem_limit_bytes=48 * 1024 * 1024
            ),
        )(logits, tokens, lengths, group_ids, rewards, old_logp, ref_logp)
        return logp, small[0, :, 0], small[1, :, 0], small[2, 0, 0]

    in_specs = (
        P("dp", None, "tensor"),
        P("dp", None),
        P("dp"),
        P("dp"),
        P("dp"),
        P("dp", None),
        P("dp", None),
    )
    out_specs = (P("dp", None), P("dp"), P("dp"), P())
    return jax.shard_map(local, mesh=mesh, in_specs=in_specs, out_specs=out_specs, check_vma=False)
```
